256 devices in a mesh: expert: 64 (over y, z, core), token: 4 (over x).
Axes of the slice: x: 4, y: 4, z: 8, core: 2. Of those that a mesh axis runs over, the one named last changes fastest.
Arguments:
- cotangent: bfloat16 [32768, 2048], P(('expert', 'token')), may hold values from -6 to 6
- expert_ids: int32 [32768, 6], P(('expert', 'token')), may hold values from 0 to 63, all different within a row; in each aligned block of 128 rows (0 to 127, 128 to 255, ...) at most 14 rows name the same one
- gate_values: float32 [32768, 6], P(('expert', 'token')), may hold values from 0.05 to 0.45
- hidden_pre: bfloat16 [64, 3584, 768], P('expert', 'token'), may hold values from -8 to 8
- up_weight: bfloat16 [64, 2048, 768], P('expert'), may hold values from -0.125 to 0.125
- down_weight: bfloat16 [64, 2048, 768], P('expert'), may hold values from -0.21875 to 0.21875
Outputs:
- input_grad: bfloat16 [32768, 2048], P(('expert', 'token'))
- down_grad: bfloat16 [64, 2048, 768], P('expert', 'token')
The draws below stay inside these ranges and needn't reach their ends.
Inputs may be any that keep to these rules, and one draw needn't show every extreme that they name: `expert_ids`: each row names 6 different experts. Among the 128 rows of one device no expert is named more than 14 times, and in every draw some expert is named exactly 14 times by the rows of some device.
All inputs are finite; a program needn't handle non-finite values.
Results may differ from the reference program's by a relative error of at most 0.007.
Values may be sent and summed in bfloat16 or wider, within the bound.
No kernel may reach another device: no remote copies, remote signals or barrier semaphores. Data moves between devices by JAX's collectives and lax.ppermute only.
A program may use at most 128 MiB of HBM per device.

```python
import math
import jax
import jax.numpy as jnp
import numpy as np
from jax import lax

D = 2048
H = 768
TOP = 6
T_DEV = 128
EXPERTS = 64
CAP = 14
SLOTS = 3584
TOKENS = 32768
N_TOKEN = 4


def steps_of(rng, extent, shards, smallest, largest):
    factor_of = 1.0
    for dim, shards_of in shards:
        steps = jax.random.uniform(jax.random.fold_in(jax.random.fold_in(rng, 6), dim), (shards_of,), jnp.float32, smallest / len(shards), largest / len(shards))
        factor_of = factor_of * jnp.repeat(jnp.exp(steps), extent[dim] // shards_of).reshape((-1,) + (1,) * (len(extent) - 1 - dim))
    return factor_of


def assign_block(rng, own, number, rows, number_of, top, reach, lean):
    ranking = jax.random.permutation(rng, number_of)
    crowded, common = shares(number_of, rows * top, reach, lean, True), shares(number_of, rows * top, reach, lean, False)
    places = jnp.arange(number_of)

    def named(tallies, offset_by):
        used = int((tallies > 0).sum())
        fixed = max(1, used // 4)
        passed = fixed + (places - fixed + offset_by * (used - fixed)) % max(1, number_of - fixed)
        return jnp.zeros((number_of,), jnp.int32).at[ranking[jnp.where(places < fixed, places, passed)]].set(jnp.asarray(tallies, jnp.int32))

    tallies = jnp.where(number % 4 == 0, named(crowded, number // 4), named(common, number - number // 4 - 1))
    mixed = jax.random.permutation(jax.random.fold_in(own, 3), number_of)
    donor, receiver = mixed[0:number_of // 2 * 2:2], mixed[1:number_of // 2 * 2:2]
    margin = jnp.minimum(tallies[donor] - 1, reach - tallies[receiver]) // 2
    margin = jnp.where((donor == ranking[0]) | (receiver == ranking[0]) | (tallies[receiver] == 0), 0, jnp.maximum(margin, 0))
    passed = jax.random.randint(jax.random.fold_in(own, 4), (number_of // 2,), 0, 1 << 20) % (margin + 1)
    tallies = tallies.at[donor].add(-passed).at[receiver].add(passed)
    members = jnp.searchsorted(jnp.cumsum(tallies), jnp.arange(rows * top), side="right").astype(jnp.int32)
    listing = members.reshape(top, rows).T
    listing = listing[jax.random.permutation(jax.random.fold_in(own, 1), rows)]
    offset_by = jax.random.randint(jax.random.fold_in(own, 2), (rows, 1), 0, top)
    return jnp.take_along_axis(listing, (jnp.arange(top)[None, :] + offset_by) % top, axis=1)


def shares(amount, total, bound, lean, full):
    loads = [(1 << 20) // math.isqrt(grade ** lean) + 1 for grade in range(1, amount + 1)]
    largest = bound if full else min(bound, max(-(-total // amount), total * loads[0] // sum(loads)))
    least = 1 if total - largest >= amount - 1 else 0
    holding, rest = [largest] + [least] * (amount - 1), total - largest - least * (amount - 1)
    while rest > 0:
        free = [i for i in range(1, amount) if holding[i] < largest] or [i for i in range(1, amount) if holding[i] < bound]
        pool, budget = sum([loads[i] for i in free]), rest
        for i in free:
            addition = min(bound - holding[i], max(1, budget * loads[i] // pool), rest)
            holding[i] = holding[i] + addition
            rest = rest - addition
    return np.array(holding)


def scatter_about(rng, dims, scale, bound, split=(), kind=jnp.bfloat16):
    factor_of = steps_of(rng, dims, split, -0.22, 0.18) if split else 1.0
    values = jax.random.normal(rng, dims, jnp.float32) * scale * factor_of
    return jnp.minimum(jnp.maximum(values, -bound), bound).astype(kind)


def setup_inputs(seed: int = 0) -> dict:
    splits = jax.random.split(jax.random.key(seed), 7)
    cotangent = scatter_about(splits[0], (TOKENS, D), 1.0, 6.0, ((0, 256),))
    expert_ids_keys = jax.random.split(jax.random.fold_in(splits[1], 1), TOKENS // T_DEV)
    expert_ids_turns = jax.random.permutation(jax.random.fold_in(splits[1], 3), TOKENS // T_DEV)
    expert_ids = jax.vmap(lambda own, number: assign_block(jax.random.fold_in(splits[1], 2), own, number, T_DEV, EXPERTS, TOP, CAP, 2))(expert_ids_keys, expert_ids_turns).reshape((TOKENS, TOP))
    gate_values = jnp.clip(0.05 + 0.39999999 * jax.random.uniform(splits[2], (TOKENS, TOP), jnp.float32) ** steps_of(splits[2], (TOKENS, TOP), ((0, 256),), -0.2, 0.2), 0.05, 0.45)
    hidden_pre = scatter_about(splits[3], (EXPERTS, SLOTS, H), 1.5, 8.0, ((0, 64), (1, 4)))
    up_weight = scatter_about(splits[4], (EXPERTS, D, H), D ** -0.5, 0.125, ((0, 64),))
    down_weight = scatter_about(splits[5], (EXPERTS, D, H), H ** -0.5, 0.21875, ((0, 64),))
    return {"cotangent": cotangent, "expert_ids": expert_ids, "gate_values": gate_values, "hidden_pre": hidden_pre, "up_weight": up_weight, "down_weight": down_weight}


grad_scale = 0.03125
root_half = 0.7071067811865476
inv_root_two_pi = 0.3989422804014327


def slope_and_act(hidden_rows):
    values = hidden_rows.astype(jnp.float32)
    normal_cdf = 0.5 * (1.0 + lax.erf(values * root_half))
    density = inv_root_two_pi * jnp.exp(-0.5 * values * values)
    slopes = normal_cdf + values * density
    active = (values * normal_cdf).astype(jnp.bfloat16)
    return slopes, active


def slot_tables(expert_ids, gate_values, slot_count):
    top_count = expert_ids.shape[1]
    blocks = expert_ids.shape[0] // T_DEV
    grouped = expert_ids.reshape(blocks, T_DEV * top_count)
    one_hot = (grouped[:, :, None] == jnp.arange(EXPERTS, dtype=jnp.int32)[None, None, :]).astype(jnp.int32)
    earlier = jnp.cumsum(one_hot, axis=1) - one_hot
    rank_in = jnp.sum(earlier * one_hot, axis=2).astype(jnp.int32)
    block_ids = jnp.arange(blocks, dtype=jnp.int32)[:, None]
    slot_row = (block_ids % N_TOKEN) * (EXPERTS * CAP) + (block_ids // N_TOKEN) * CAP + rank_in
    token_ids = block_ids * T_DEV + jnp.arange(T_DEV * top_count, dtype=jnp.int32)[None, :] // top_count
    flat_expert = grouped.reshape(-1).astype(jnp.int32)
    flat_slot = slot_row.reshape(-1).astype(jnp.int32)
    slot_token = jnp.zeros((EXPERTS, slot_count), jnp.int32).at[flat_expert, flat_slot].set(token_ids.reshape(-1).astype(jnp.int32))
    slot_gate = jnp.zeros((EXPERTS, slot_count), jnp.float32).at[flat_expert, flat_slot].set(gate_values.reshape(-1))
    slot_live = jnp.zeros((EXPERTS, slot_count), jnp.float32).at[flat_expert, flat_slot].set(jnp.ones_like(gate_values.reshape(-1)))
    return slot_token, slot_gate, slot_live


def apply_transpose(token_rows, slot_token, slot_gate, slot_live, hidden_pre, up_weight, down_weight):
    def per_expert(summed, stacked):
        token_ids, gate_e, live_e, hidden_e, up_e, down_e = stacked
        slopes, unused_act = slope_and_act(hidden_e)
        gathered = jnp.take(token_rows, token_ids, axis=0)
        gathered = jnp.where(live_e[:, None] > 0.5, gathered, jnp.zeros_like(gathered))
        inner_prod = jnp.dot(gathered, down_e, preferred_element_type=jnp.float32)
        scaled = (inner_prod * slopes).astype(jnp.bfloat16)
        pieces = jnp.dot(scaled, up_e.T, preferred_element_type=jnp.float32).astype(jnp.bfloat16)
        weighted = pieces.astype(jnp.float32) * gate_e[:, None]
        summed = summed.at[token_ids].add(weighted)
        return summed, jnp.zeros((), jnp.float32)

    initial = jnp.zeros(token_rows.shape, jnp.float32)
    summed, unused_out = lax.scan(per_expert, initial, (slot_token, slot_gate, slot_live, hidden_pre, up_weight, down_weight))
    return summed.astype(jnp.bfloat16)


def reference(cotangent, expert_ids, gate_values, hidden_pre, up_weight, down_weight):
    slot_token, slot_gate, slot_live = slot_tables(expert_ids, gate_values, hidden_pre.shape[1])
    first_term = apply_transpose(cotangent, slot_token, slot_gate, slot_live, hidden_pre, up_weight, down_weight)
    second = apply_transpose(first_term, slot_token, slot_gate, slot_live, hidden_pre, up_weight, down_weight)
    input_grad = (cotangent.astype(jnp.float32) + first_term.astype(jnp.float32) + second.astype(jnp.float32)).astype(jnp.bfloat16)

    def grad_expert(carried, stacked):
        token_ids, gate_e, hidden_e = stacked
        unused_slope, active = slope_and_act(hidden_e)
        picked = jnp.take(input_grad, token_ids, axis=0).astype(jnp.float32)
        routed = (picked * gate_e[:, None]).astype(jnp.bfloat16)
        grad_e = jnp.dot(routed.T, active, preferred_element_type=jnp.float32)
        return carried, (grad_e * grad_scale).astype(jnp.bfloat16)

    unused_carry, down_grad = lax.scan(grad_expert, jnp.zeros((), jnp.float32), (slot_token, slot_gate, hidden_pre))
    return input_grad, down_grad
```

```python
import jax
import jax.numpy as jnp
from jax import lax
from jax.experimental import pallas as pl
from jax.experimental.pallas import tpu as pltpu
from jax.sharding import Mesh, PartitionSpec as P

grad_scale = 0.03125
root_half = 0.7071067811865476
inv_root_two_pi = 0.3989422804014327

USE_KERNELS = True
bf16 = jnp.bfloat16
f32 = jnp.float32
vmem = pl.BlockSpec(memory_space=pltpu.VMEM)


def slope_and_act(hidden_rows):
    values = hidden_rows.astype(f32)
    normal_cdf = 0.5 * (1.0 + lax.erf(values * root_half))
    density = inv_root_two_pi * jnp.exp(-0.5 * values * values)
    slopes = normal_cdf + values * density
    return slopes, (values * normal_cdf).astype(bf16)


def expert_in(arrived, down, slopes):
    ny, halves, per, width = arrived.shape
    hidden = down.shape[2]
    if not USE_KERNELS:
        inner = jnp.einsum("yhrw,hwk->yrk", arrived, down, preferred_element_type=f32)
        return (inner.reshape(ny * per, hidden) * slopes).astype(bf16)

    def kernel(arrived_ref, down_ref, slope_ref, out_ref, joined):
        total = None
        for h in range(halves):
            for y in range(ny):
                joined[h, y * per : (y + 1) * per, :] = arrived_ref[y, h]
            part = jnp.dot(joined[h], down_ref[h], preferred_element_type=f32)
            total = part if total is None else total + part
        out_ref[...] = (total * slope_ref[...]).astype(bf16)

    return pl.pallas_call(
        kernel,
        out_shape=jax.ShapeDtypeStruct((ny * per, hidden), bf16),
        in_specs=[vmem] * 3,
        out_specs=vmem,
        scratch_shapes=[pltpu.VMEM((halves, ny * per, width), bf16)],
        cost_estimate=pl.CostEstimate(
            flops=2 * ny * per * halves * width * hidden,
            transcendentals=0,
            bytes_accessed=2 * (arrived.size + down.size) + 6 * ny * per * hidden,
        ),
    )(arrived, down, slopes)


def expert_out(scaled, up, ny):
    halves, width, hidden = up.shape
    per = scaled.shape[0] // ny
    if not USE_KERNELS:
        out = jnp.einsum("yrk,hwk->yhrw", scaled.reshape(ny, per, hidden), up, preferred_element_type=f32)
        return out.astype(bf16)

    def kernel(scaled_ref, up_ref, out_ref):
        for h in range(halves):
            part = lax.dot_general(
                scaled_ref[...], up_ref[h], (((1,), (1,)), ((), ())), preferred_element_type=f32
            )
            for y in range(ny):
                out_ref[y, h] = part[y * per : (y + 1) * per, :].astype(bf16)

    return pl.pallas_call(
        kernel,
        out_shape=jax.ShapeDtypeStruct((ny, halves, per, width), bf16),
        in_specs=[vmem] * 2,
        out_specs=vmem,
        cost_estimate=pl.CostEstimate(
            flops=2 * scaled.size * halves * width,
            transcendentals=0,
            bytes_accessed=2 * (scaled.size + up.size + scaled.shape[0] * halves * width),
        ),
    )(scaled, up)


def gradient(arrived, actives, total, last):
    ny, halves, nt, per, width = arrived.shape
    hidden = actives.shape[2]
    finish = lambda value: (value * grad_scale).astype(bf16) if last else value
    if not USE_KERNELS:
        acts = actives.reshape(nt, ny, per, hidden)
        out = jnp.einsum("yhtrw,tyrk->hwk", arrived, acts, preferred_element_type=f32)
        out = out.reshape(halves * width, hidden)
        return finish(out if total is None else out + total)

    def kernel(*refs):
        arrived_ref, active_ref = refs[:2]
        total_ref = refs[2] if total is not None else None
        out_ref, joined = refs[-2:]
        for h in range(halves):
            for t in range(nt):
                for y in range(ny):
                    at = (t * ny + y) * per
                    joined[at : at + per, :] = arrived_ref[y, h, t]
            part = lax.dot_general(
                joined[...], active_ref[...].reshape(nt * ny * per, hidden), (((0,), (0,)), ((), ())),
                preferred_element_type=f32,
            )
            rows = slice(h * width, (h + 1) * width)
            if total is not None:
                part = part + total_ref[rows, :]
            out_ref[rows, :] = finish(part)

    extra = [] if total is None else [total]
    return pl.pallas_call(
        kernel,
        out_shape=jax.ShapeDtypeStruct((halves * width, hidden), bf16 if last else f32),
        in_specs=[vmem] * (2 + len(extra)),
        out_specs=vmem,
        scratch_shapes=[pltpu.VMEM((nt * ny * per, width), bf16)],
        cost_estimate=pl.CostEstimate(
            flops=2 * arrived.size * hidden,
            transcendentals=0,
            bytes_accessed=2 * (arrived.size + actives.size) + 8 * halves * width * hidden,
        ),
    )(arrived, actives, *extra)


def body(cotangent, expert_ids, gate_values, hidden_pre, up_weight, down_weight):
    ny, nz, nc, nx = (lax.axis_size(a) for a in ("y", "z", "c", "x"))
    z = lax.axis_index("z")
    experts = ny * nz * nc
    tokens, top = expert_ids.shape
    width = cotangent.shape[1]
    slots = hidden_pre.shape[1]
    cap = slots // experts
    per = nz * cap
    part = width // nx // nc

    def halves_of(weight):
        rows = weight.reshape(nx, nc, part, weight.shape[1])
        return jnp.swapaxes(rows, 0, 1).reshape(nc, nx * part, weight.shape[1])

    up, down = halves_of(up_weight[0]), halves_of(down_weight[0])

    def swap(value):
        return lax.all_to_all(value, "c", split_axis=0, concat_axis=0, tiled=True)

    shaped = jnp.moveaxis(cotangent.reshape(tokens, nx, nc, part), 2, 0).reshape(nc, tokens, nx * part)
    start = swap(shaped)

    routes = expert_ids.reshape(-1)
    one_hot = (routes[:, None] == jnp.arange(experts, dtype=jnp.int32)[None, :]).astype(jnp.int32)
    earlier = jnp.cumsum(one_hot, axis=0) - one_hot
    rank = jnp.sum(earlier * one_hot, axis=1)
    code = (routes * cap + rank).reshape(tokens, top)
    meta = jnp.concatenate([code.astype(f32), gate_values], 1).T
    peers = nz * nc * nx
    meta = lax.all_to_all(
        jnp.broadcast_to(meta[None], (peers,) + meta.shape), ("z", "c", "x"), split_axis=0, concat_axis=0, tiled=True
    ).reshape(nz, nc, nx, 2 * top, tokens)
    steps = jnp.arange(nz)
    near = jnp.arange(ny * nc)
    expert_of = (near // nc * nz + z) * nc + near % nc
    row_code = (
        expert_of[:, None, None] * cap + steps[None, :, None] * slots + jnp.arange(cap)[None, None, :]
    ).reshape(slots, 1)
    column_code = meta[:, :, :, :top].astype(jnp.int32) + steps[:, None, None, None, None] * slots
    column_gate = meta[:, :, :, top:]
    own_x = lax.axis_index("x")

    def pick_table(codes, gates):
        codes = jnp.moveaxis(codes, 1, 0).reshape(top, 1, nz * tokens)
        gates = jnp.moveaxis(gates, 1, 0).reshape(top, 1, nz * tokens)
        pick = jnp.zeros((slots, nz * tokens), f32)
        gated = jnp.zeros((slots, nz * tokens), f32)
        for k in range(top):
            match = row_code == codes[k]
            pick = pick + match.astype(f32)
            gated = gated + jnp.where(match, gates[k], 0.0)
        return pick.astype(bf16), jnp.sum(gated, axis=1, keepdims=True)

    def combine_table(codes, gates):
        codes = jnp.moveaxis(codes, 2, 1).reshape(nz * tokens, top)
        gates = jnp.moveaxis(gates, 2, 1).reshape(nz * tokens, top)
        total = jnp.zeros((nz * tokens, slots), f32)
        for k in range(top):
            total = total + jnp.where(codes[:, k : k + 1] == row_code.reshape(1, slots), gates[:, k : k + 1], 0.0)
        return total.astype(bf16)

    here = lambda values, s: lax.dynamic_index_in_dim(values[:, s], own_x, 1, keepdims=False)
    picks = [pick_table(here(column_code, s), here(column_gate, s))[0] for s in range(nc)]
    combines = [combine_table(here(column_code, s), here(column_gate, s)) for s in range(nc)]

    hidden = hidden_pre[0].reshape(ny * nz, nc, cap, hidden_pre.shape[2])
    slopes, actives = [], []
    for s in range(nc):
        slope, active = slope_and_act(hidden[:, s].reshape(ny * per, -1))
        slopes.append(slope)
        actives.append(active)
    both = jnp.stack(actives)
    all_actives = [both]
    for dx in range(1, nx):
        with jax.named_scope(f"act{dx}"):
            all_actives.append(lax.ppermute(both, "x", [(i, (i - dx) % nx) for i in range(nx)]))

    def across(rows):
        return lax.all_to_all(rows, ("y", "c"), split_axis=0, concat_axis=0, tiled=True)

    def gather(block):
        return lax.all_gather(block, "z", axis=0, tiled=True)

    def jacobian(block, s):
        with jax.named_scope(f"gz{s}"):
            rows = gather(block)
        rows = jnp.dot(picks[s], rows, preferred_element_type=f32).astype(bf16)
        with jax.named_scope(f"dy{s}"):
            arrived = across(rows.reshape(ny * nc, per, -1)).reshape(ny, nc, per, -1)
        scaled = expert_in(arrived, down, slopes[s])
        pieces = expert_out(scaled, up, ny)
        with jax.named_scope(f"ry{s}"):
            returned = across(pieces.reshape(ny * nc, per, -1)).reshape(slots, -1)
        parts = jnp.dot(combines[s], returned, preferred_element_type=f32).astype(bf16)
        with jax.named_scope(f"sz{s}"):
            return lax.psum_scatter(parts, "z", scatter_dimension=0, tiled=True)

    first = [jacobian(start[s], s) for s in range(nc)]
    second = [jacobian(first[s], s) for s in range(nc)]
    grads = [
        (start[s].astype(f32) + first[s].astype(f32) + second[s].astype(f32)).astype(bf16) for s in range(nc)
    ]
    own = swap(jnp.stack(grads))
    input_grad = jnp.moveaxis(own.reshape(nc, tokens, nx, part), 0, 2).reshape(tokens, width)

    total = None
    rolled_code = jnp.take(column_code, (own_x + jnp.arange(nx)) % nx, axis=2)
    rolled_gate = jnp.take(column_gate, (own_x + jnp.arange(nx)) % nx, axis=2)
    for s in range(nc):
        columns = jnp.moveaxis(grads[s].reshape(tokens, nx, part), 1, 0)
        with jax.named_scope(f"igx{s}"):
            owned = lax.all_to_all(columns, "x", split_axis=0, concat_axis=0, tiled=True)
        owned = jnp.take(owned, (own_x + jnp.arange(nx)) % nx, axis=0)
        with jax.named_scope(f"ez{s}"):
            spread = gather(owned.reshape(nx * tokens, part)).reshape(nz, nx, tokens, part)
        rows = []
        for dx in range(nx):
            pick, gate = pick_table(rolled_code[:, s, dx], rolled_gate[:, s, dx])
            row = jnp.dot(pick, spread[:, dx].reshape(nz * tokens, part), preferred_element_type=f32)
            rows.append((row * gate).astype(bf16).reshape(ny * nc, 1, per, part))
        with jax.named_scope(f"ey{s}"):
            arrived = across(jnp.concatenate(rows, 1)).reshape(ny, nc, nx, per, part)
        acts = jnp.stack([a[s] for a in all_actives])
        total = gradient(arrived, acts, total, s == nc - 1)
    return input_grad, total[None]


def solution(mesh):
    axes = ("y", "z", "c", "x")
    count_z, count_c = 8, 2
    grid = mesh.devices.reshape(-1, count_z, count_c, mesh.devices.shape[1])
    inner_mesh = Mesh(grid, axes)
    in_specs = (
        P(axes, None),
        P(axes, None),
        P(axes, None),
        P(axes[:3], "x", None),
        P(axes[:3], None, None),
        P(axes[:3], None, None),
    )
    out_specs = (P(axes, None), P(axes[:3], "x", None))
    return jax.shard_map(body, mesh=inner_mesh, in_specs=in_specs, out_specs=out_specs, check_vma=False)
```

```python
import jax
import jax.numpy as jnp
from jax import lax
from jax.experimental import pallas as pl
from jax.experimental.pallas import tpu as pltpu
from jax.sharding import Mesh, PartitionSpec as P

grad_scale = 0.03125
root_half = 0.7071067811865476
inv_root_two_pi = 0.3989422804014327

USE_KERNELS = True
bf16 = jnp.bfloat16
f32 = jnp.float32
vmem = pl.BlockSpec(memory_space=pltpu.VMEM)


def slope_and_act(hidden_rows):
    values = hidden_rows.astype(f32)
    normal_cdf = 0.5 * (1.0 + lax.erf(values * root_half))
    density = inv_root_two_pi * jnp.exp(-0.5 * values * values)
    slopes = normal_cdf + values * density
    return slopes, (values * normal_cdf).astype(bf16)


def tie(value, earlier):
    return lax.optimization_barrier((value, earlier))[0]


def table_matmul(tables, blocks, rows, split):
    count, height, depth = tables.shape
    each, width = blocks[0].shape[1:]
    groups = height // rows
    if not USE_KERNELS:
        out = jnp.einsum("trd,tdw->trw", tables, jnp.concatenate(blocks, 1), preferred_element_type=f32)
        out = jnp.swapaxes(out.astype(bf16).reshape(count, groups, rows, width), 0, 1)
        return [out[i] for i in range(groups)] if split else out
    step = min(width, 256)

    def kernel(*refs):
        table_ref, block_refs = refs[0], refs[1 : 1 + len(blocks)]
        out_refs, joined = refs[1 + len(blocks) : -1], refs[-1]
        for j, ref in enumerate(block_refs):
            joined[j * each : (j + 1) * each, :] = ref[0]
        product = jnp.dot(table_ref[0], joined[...], preferred_element_type=f32)
        for i in range(groups):
            part = product[i * rows : (i + 1) * rows, :].astype(bf16)
            if split:
                out_refs[i][0] = part
            else:
                out_refs[0][i, 0] = part

    if split:
        out_shape = [jax.ShapeDtypeStruct((count, rows, width), bf16)] * groups
        out_specs = [pl.BlockSpec((1, rows, step), lambda t, i: (t, 0, i))] * groups
    else:
        out_shape = jax.ShapeDtypeStruct((groups, count, rows, width), bf16)
        out_specs = pl.BlockSpec((groups, 1, rows, step), lambda t, i: (0, t, 0, i))
    return pl.pallas_call(
        kernel,
        grid=(count, width // step),
        out_shape=out_shape,
        in_specs=[pl.BlockSpec((1, height, depth), lambda t, i: (t, 0, 0))]
        + [pl.BlockSpec((1, each, step), lambda t, i: (t, 0, i))] * len(blocks),
        out_specs=out_specs,
        scratch_shapes=[pltpu.VMEM((depth, step), bf16)],
        cost_estimate=pl.CostEstimate(
            flops=2 * tables.size * width,
            transcendentals=0,
            bytes_accessed=2 * (tables.size + count * (depth + height) * width),
        ),
    )(tables, *blocks)


def expert_in(arrived, down, slopes):
    halves, width, hidden = down.shape
    split = isinstance(arrived, list)
    per = arrived[0].shape[0] if split else arrived.shape[1]
    count = slopes.shape[0] // per * halves
    if not USE_KERNELS:
        whole = (jnp.stack(arrived) if split else arrived).reshape(count // halves, halves, per, width)
        inner = jnp.einsum("yhrw,hwk->yrk", whole, down, preferred_element_type=f32)
        return (inner.reshape(-1, hidden) * slopes).astype(bf16)
    step = width // 4
    last = 3

    def kernel(*refs):
        arrived_refs, (down_ref, slope_ref, out_ref, joined, total) = refs[:-5], refs[-5:]
        at = pl.program_id(0)
        part = None
        for h in range(halves):
            for y in range(count // halves):
                i = y * halves + h
                joined[h, y * per : (y + 1) * per, :] = arrived_refs[i][...] if split else arrived_refs[0][i]
            more = jnp.dot(joined[h], down_ref[h], preferred_element_type=f32)
            part = more if part is None else part + more

        @pl.when(at == 0)
        def _():
            total[...] = part

        @pl.when((at > 0) & (at < last))
        def _():
            total[...] += part

        @pl.when(at == last)
        def _():
            out_ref[...] = ((total[...] + part) * slope_ref[...]).astype(bf16)

    if split:
        specs, operands = [pl.BlockSpec((per, step), lambda i: (0, i))] * count, arrived
    else:
        specs, operands = [pl.BlockSpec((count, per, step), lambda i: (0, 0, i))], [arrived]
    return pl.pallas_call(
        kernel,
        grid=(4,),
        out_shape=jax.ShapeDtypeStruct(slopes.shape, bf16),
        in_specs=specs
        + [
            pl.BlockSpec((halves, step, hidden), lambda i: (0, i, 0)),
            pl.BlockSpec(slopes.shape, lambda i: (0, 0)),
        ],
        out_specs=pl.BlockSpec(slopes.shape, lambda i: (0, 0)),
        scratch_shapes=[pltpu.VMEM((halves, count // halves * per, step), bf16), pltpu.VMEM(slopes.shape, f32)],
        cost_estimate=pl.CostEstimate(
            flops=2 * slopes.size * halves * width,
            transcendentals=0,
            bytes_accessed=2 * (count * per * width + down.size) + 6 * slopes.size,
        ),
    )(*operands, down, slopes)


def expert_out(scaled, up, per, split):
    halves, width, hidden = up.shape
    ny = scaled.shape[0] // per
    count = ny * halves
    if not USE_KERNELS:
        out = jnp.einsum("yrk,hwk->yhrw", scaled.reshape(ny, per, hidden), up, preferred_element_type=f32)
        out = out.astype(bf16).reshape(count, per, width)
        return [out[i] for i in range(count)] if split else out
    step = width // 4

    def kernel(scaled_ref, up_ref, *out_refs):
        for h in range(halves):
            part = lax.dot_general(
                scaled_ref[...], up_ref[h], (((1,), (1,)), ((), ())), preferred_element_type=f32
            )
            for y in range(ny):
                rows = part[y * per : (y + 1) * per, :].astype(bf16)
                if split:
                    out_refs[y * halves + h][...] = rows
                else:
                    out_refs[0][y * halves + h] = rows

    if split:
        out_shape = [jax.ShapeDtypeStruct((per, width), bf16)] * count
        out_specs = [pl.BlockSpec((per, step), lambda i: (0, i))] * count
    else:
        out_shape = jax.ShapeDtypeStruct((count, per, width), bf16)
        out_specs = pl.BlockSpec((count, per, step), lambda i: (0, 0, i))
    return pl.pallas_call(
        kernel,
        grid=(4,),
        out_shape=out_shape,
        in_specs=[
            pl.BlockSpec(scaled.shape, lambda i: (0, 0)),
            pl.BlockSpec((halves, step, hidden), lambda i: (0, i, 0)),
        ],
        out_specs=out_specs,
        cost_estimate=pl.CostEstimate(
            flops=2 * scaled.size * halves * width,
            transcendentals=0,
            bytes_accessed=2 * (scaled.size + up.size + count * per * width),
        ),
    )(scaled, up)


def gradient(arrived, actives, total, last):
    split = isinstance(arrived, list)
    nt, per, width = arrived[0].shape if split else arrived.shape[1:]
    hidden = actives.shape[2]
    ny = actives.shape[1] // per
    count = len(arrived) if split else arrived.shape[0]
    halves = count // ny
    finish = lambda value: (value * grad_scale).astype(bf16) if last else value
    if not USE_KERNELS:
        whole = (jnp.stack(arrived) if split else arrived).reshape(ny, halves, nt, per, width)
        acts = actives.reshape(nt, ny, per, hidden)
        out = jnp.einsum("yhtrw,tyrk->hwk", whole, acts, preferred_element_type=f32)
        out = out.reshape(halves * width, hidden)
        return finish(out if total is None else out + total)

    def kernel(*refs):
        arrived_refs = refs[: count if split else 1]
        active_ref = refs[len(arrived_refs)]
        total_ref = refs[len(arrived_refs) + 1] if total is not None else None
        out_ref, joined = refs[-2:]
        for h in range(halves):
            for t in range(nt):
                for y in range(ny):
                    at = (t * ny + y) * per
                    i = y * halves + h
                    joined[at : at + per, :] = arrived_refs[i][t] if split else arrived_refs[0][i, t]
            part = lax.dot_general(
                joined[...], active_ref[...].reshape(nt * ny * per, hidden), (((0,), (0,)), ((), ())),
                preferred_element_type=f32,
            )
            rows = slice(h * width, (h + 1) * width)
            if total is not None:
                part = part + total_ref[rows, :]
            out_ref[rows, :] = finish(part)

    operands = (arrived if split else [arrived]) + [actives] + ([] if total is None else [total])
    return pl.pallas_call(
        kernel,
        out_shape=jax.ShapeDtypeStruct((halves * width, hidden), bf16 if last else f32),
        in_specs=[vmem] * len(operands),
        out_specs=vmem,
        scratch_shapes=[pltpu.VMEM((nt * ny * per, width), bf16)],
        cost_estimate=pl.CostEstimate(
            flops=2 * count * nt * per * width * hidden,
            transcendentals=0,
            bytes_accessed=2 * (count * nt * per * width + actives.size) + 8 * halves * width * hidden,
        ),
    )(*operands)


def shift(value, axis, by, name):
    size = lax.axis_size(axis)
    with jax.named_scope(name):
        return lax.ppermute(value, axis, [(i, (i + by) % size) for i in range(size)])


def exchange(blocks, sign, name):
    ny, nc = lax.axis_size("y"), lax.axis_size("c")
    out = [blocks[0]]
    for i in range(1, len(blocks)):
        dy, dc = i // nc, i % nc
        pairs = [
            (y * nc + c, (y + sign * dy) % ny * nc + (c + dc) % nc) for y in range(ny) for c in range(nc)
        ]
        with jax.named_scope(f"{name}{i}"):
            out.append(lax.ppermute(blocks[i], ("y", "c"), pairs))
    return out


def gather_ring(block, odd, name):
    size = lax.axis_size("z")
    out = [block] + [None] * (size - 1)
    ahead = size // 2 - odd
    held = back = block
    for s in range(1, size // 2 + 1):
        if s <= ahead:
            held = out[size - s] = shift(held, "z", 1, f"{name}f{s}")
        if s <= size - 1 - ahead:
            back = out[s] = shift(back, "z", -1, f"{name}b{s}")
    return out


def scatter_ring(blocks, odd, name):
    size = lax.axis_size("z")
    ahead = size // 2 - odd
    add = lambda a, b: (a.astype(f32) + b.astype(f32)).astype(bf16)
    held, back = blocks[ahead], blocks[ahead + 1]
    for s in range(1, size // 2 + 1):
        if s <= ahead:
            held = shift(held, "z", 1, f"{name}f{s}")
            if ahead - s > 0:
                held = add(held, blocks[ahead - s])
        if s <= size - 1 - ahead:
            back = shift(back, "z", -1, f"{name}b{s}")
            if ahead + 1 + s < size:
                back = add(back, blocks[ahead + 1 + s])
    return (held.astype(f32) + back.astype(f32) + blocks[0].astype(f32)).astype(bf16)


def body(cotangent, expert_ids, gate_values, hidden_pre, up_weight, down_weight):
    ny, nz, nc, nx = (lax.axis_size(a) for a in ("y", "z", "c", "x"))
    own_y, own_z, own_c, own_x = (lax.axis_index(a) for a in ("y", "z", "c", "x"))
    experts = ny * nz * nc
    tokens, top = expert_ids.shape
    width = cotangent.shape[1]
    slots = hidden_pre.shape[1]
    cap = slots // experts
    per = nz * cap
    part = width // nx // nc
    RING = 1

    def halves_of(weight):
        rows = weight.reshape(nx, nc, part, weight.shape[1])
        return jnp.swapaxes(rows, 0, 1).reshape(nc, nx * part, weight.shape[1])

    ups, downs = [halves_of(up_weight[0])], [halves_of(down_weight[0])]
    halves = (own_c + jnp.arange(nc)) % nc
    ups.append(jnp.take(ups[0], halves, axis=0))
    downs.append(jnp.take(downs[0], halves, axis=0))

    def swap(value):
        return lax.all_to_all(value, "c", split_axis=0, concat_axis=0, tiled=True)

    shaped = jnp.moveaxis(cotangent.reshape(tokens, nx, nc, part), 2, 0).reshape(nc, tokens, nx * part)
    start = swap(shaped)

    routes = expert_ids.reshape(-1)
    one_hot = (routes[:, None] == jnp.arange(experts, dtype=jnp.int32)[None, :]).astype(jnp.int32)
    earlier = jnp.cumsum(one_hot, axis=0) - one_hot
    rank = jnp.sum(earlier * one_hot, axis=1)
    code = (routes * cap + rank).reshape(tokens, top)
    meta = jnp.concatenate([code.astype(f32), gate_values], 1).T
    meta = lax.all_to_all(
        jnp.broadcast_to(meta[None], (nz * nc,) + meta.shape), ("z", "c"), split_axis=0, concat_axis=0, tiled=True
    )
    steps = jnp.arange(nz)
    near = jnp.arange(ny * nc)

    def row_codes(s):
        expert_y, expert_c = near // nc, near % nc
        if s == RING:
            expert_y, expert_c = (own_y + expert_y) % ny, (own_c + expert_c) % nc
        expert_of = (expert_y * nz + own_z) * nc + expert_c
        return (
            expert_of[:, None, None] * cap + steps[None, :, None] * slots + jnp.arange(cap)[None, None, :]
        ).reshape(slots, 1)

    def column_side(values, s):
        values = values.reshape(nz, nc, 2 * top, tokens)[:, s]
        codes = values[:, :top].astype(jnp.int32) + steps[:, None, None] * slots
        gates = values[:, top:]
        if s == RING:
            order = (own_z + steps) % nz
            codes, gates = jnp.take(codes, order, axis=0), jnp.take(gates, order, axis=0)
        return codes, gates

    def pick_table(values, s, gated):
        sides = [column_side(v, s) for v in values]
        codes = jnp.stack([jnp.moveaxis(c, 1, 0).reshape(top, 1, nz * tokens) for c, _ in sides])
        gates = jnp.stack([jnp.moveaxis(g, 1, 0).reshape(top, 1, nz * tokens) for _, g in sides])
        row_code = row_codes(s)[None]
        total = jnp.zeros((len(sides), slots, nz * tokens), f32)
        for k in range(top):
            match = row_code == codes[:, k]
            total = total + (jnp.where(match, gates[:, k], 0.0) if gated else match.astype(f32))
        return total.astype(bf16)

    def combine_table(values, s):
        codes, gates = column_side(values, s)
        codes = jnp.moveaxis(codes, 2, 1).reshape(nz * tokens, top)
        gates = jnp.moveaxis(gates, 2, 1).reshape(nz * tokens, top)
        row_code = row_codes(s).reshape(1, slots)
        total = jnp.zeros((nz * tokens, slots), f32)
        for k in range(top):
            total = total + jnp.where(codes[:, k : k + 1] == row_code, gates[:, k : k + 1], 0.0)
        return total.astype(bf16)[None]

    A, B = 0, 1
    picks = [pick_table([meta], s, False) for s in range(nc)]
    combines = [combine_table(meta, s) for s in range(nc)]

    hidden = hidden_pre[0].reshape(ny, nz, nc, cap, hidden_pre.shape[2])
    slopes, actives = [], []
    for s in range(nc):
        rows = hidden[:, :, s]
        if s == RING:
            rows = jnp.take(rows, (own_y - jnp.arange(ny)) % ny, axis=0)
        slope, active = slope_and_act(rows.reshape(ny * per, -1))
        slopes.append(slope)
        actives.append(active)

    def across(rows, sign, s, name):
        if s == RING:
            return exchange(rows, sign, name)
        with jax.named_scope(name):
            return lax.all_to_all(rows, ("y", "c"), split_axis=0, concat_axis=0, tiled=True)

    def gather(block, s, name):
        if s == RING:
            return gather_ring(block, 0, name)
        with jax.named_scope(name):
            return [lax.all_gather(block, "z", axis=0, tiled=True)]

    def scatter(parts, s, name):
        if s == RING:
            return scatter_ring([p[0] for p in parts], 1, name)
        with jax.named_scope(name):
            return lax.psum_scatter(parts.reshape(nz * tokens, -1), "z", scatter_dimension=0, tiled=True)

    def take_rows(s, spread, after):
        spread = [tie(block, after)[None] for block in spread] if after is not None else [b[None] for b in spread]
        rows = table_matmul(picks[s], spread, per, s == RING)
        return [r[0] for r in rows] if s == RING else rows.reshape(ny * nc, per, -1)

    def apply_expert(s, sent, after):
        scaled = expert_in(tie(sent, after), downs[s], slopes[s])
        return expert_out(scaled, ups[s], per, s == RING)

    def merge(s, back, after):
        back = tie(back, after)
        blocks = [b[None] for b in back] if s == RING else [back.reshape(1, slots, -1)]
        return table_matmul(combines[s], blocks, tokens, s == RING)

    def both_chains(spread, name, before, extra):
        rows_a = take_rows(A, spread[A], before)
        sent_a = across(rows_a, 1, A, f"{name}dya")
        pieces_a = apply_expert(A, sent_a, rows_a)
        back_a = across(pieces_a, -1, A, f"{name}rya")
        rows_b = take_rows(B, spread[B], (pieces_a, extra(rows_a)))
        sent_b = across(rows_b, 1, B, f"{name}dyb")
        parts_a = merge(A, back_a, rows_b)
        out_a = scatter(parts_a, A, f"{name}sza")
        pieces_b = apply_expert(B, sent_b, parts_a)
        back_b = across(pieces_b, -1, B, f"{name}ryb")
        parts_b = merge(B, back_b, pieces_b)
        out_b = scatter(parts_b, B, f"{name}szb")
        return [out_a, out_b], parts_b

    later = {}

    def prepare(rows):
        values = tie(meta, rows)
        far = lax.all_to_all(
            jnp.broadcast_to(values.reshape(1, -1, tokens), (nx, values.size // tokens, tokens)), "x",
            split_axis=0, concat_axis=0, tiled=True,
        )
        far = jnp.take(far, (own_x + jnp.arange(nx)) % nx, axis=0)
        both = tie(jnp.stack(actives), far)
        acts = [both] + [shift(both, "x", -dx, f"act{dx}") for dx in range(1, nx)]
        later["acts"] = [jnp.stack([a[s] for a in acts]) for s in range(nc)]
        later["far"] = far
        return far

    spread = [gather(start[A], A, "agza"), None]
    with jax.named_scope("agzb"):
        whole = lax.all_gather(tie(start[B], meta), "z", axis=0, tiled=True).reshape(nz, tokens, -1)
    spread[B] = [jnp.take(whole, (own_z + steps) % nz, axis=0).reshape(nz * tokens, -1)]
    first, last = both_chains(spread, "a", None, prepare)
    spread = [gather(first[A], A, "bgza"), gather(first[B], B, "bgzb")]
    far_picks = {}

    def make_far(rows):
        values = tie(later["far"], rows)
        for s in range(nc):
            far_picks[s] = pick_table([values[dx] for dx in range(nx)], s, True)
        return rows

    second, last = both_chains(spread, "b", (last, later["acts"]), make_far)

    own_grads, spread = [], []
    for s in range(nc):
        grad = (start[s].astype(f32) + first[s].astype(f32) + second[s].astype(f32)).astype(bf16)
        own_grads.append(grad)
        columns = jnp.moveaxis(grad.reshape(tokens, nx, part), 1, 0)
        with jax.named_scope(f"igx{s}"):
            owned = lax.all_to_all(columns, "x", split_axis=0, concat_axis=0, tiled=True)
        owned = jnp.take(owned, (own_x + jnp.arange(nx)) % nx, axis=0)
        spread.append(gather(owned.reshape(nx * tokens, part), s, f"ez{s}"))
    own = swap(jnp.stack(own_grads))
    input_grad = jnp.moveaxis(own.reshape(nc, tokens, nx, part), 0, 2).reshape(tokens, width)
    arrived = []
    for s in range(nc):
        if s == RING:
            blocks = [b.reshape(nx, tokens, part) for b in spread[s]]
        else:
            blocks = list(spread[s][0].reshape(nz, nx, tokens, part))
        rows = table_matmul(far_picks[s], blocks, per, s == RING)
        if s != RING:
            rows = rows.reshape(ny * nc, nx * per, part)
        got = across(rows, 1, s, f"ey{s}")
        arrived.append(got if s == RING else got.reshape(ny * nc, nx, per, part))
    total = gradient(arrived[A], later["acts"][A], None, False)
    total = jnp.take(total.reshape(nc, nx * part // nx, -1), halves, axis=0).reshape(total.shape)
    total = gradient(arrived[B], later["acts"][B], total, True)
    total = jnp.take(total.reshape(nc, part, -1), halves, axis=0).reshape(total.shape)
    return input_grad, total[None]


def solution(mesh):
    axes = ("y", "z", "c", "x")
    count_z, count_c = 8, 2
    grid = mesh.devices.reshape(-1, count_z, count_c, mesh.devices.shape[1])
    inner_mesh = Mesh(grid, axes)
    in_specs = (
        P(axes, None),
        P(axes, None),
        P(axes, None),
        P(axes[:3], "x", None),
        P(axes[:3], None, None),
        P(axes[:3], None, None),
    )
    out_specs = (P(axes, None), P(axes[:3], "x", None))
    return jax.shard_map(body, mesh=inner_mesh, in_specs=in_specs, out_specs=out_specs, check_vma=False)
```

```python
import jax
import jax.numpy as jnp
from jax import lax
from jax.experimental import pallas as pl
from jax.experimental.pallas import tpu as pltpu
from jax.sharding import Mesh, PartitionSpec as P


grad_scale = 0.03125
root_half = 0.7071067811865476
inv_root_two_pi = 0.3989422804014327

USE_KERNELS = True
bf16 = jnp.bfloat16
f32 = jnp.float32
vmem = pl.BlockSpec(memory_space=pltpu.VMEM)
smem = pl.BlockSpec(memory_space=pltpu.SMEM)


def slope_and_act(hidden_rows):
    values = hidden_rows.astype(f32)
    normal_cdf = 0.5 * (1.0 + lax.erf(values * root_half))
    density = inv_root_two_pi * jnp.exp(-0.5 * values * values)
    slopes = normal_cdf + values * density
    return slopes, (values * normal_cdf).astype(bf16)


def tie(value, earlier):
    return lax.optimization_barrier((value, earlier))[0]


def table_matmul(tables, blocks, rows, split):
    count, height, depth = tables.shape
    each, width = blocks[0].shape[1:]
    groups = height // rows
    if not USE_KERNELS:
        out = jnp.einsum("trd,tdw->trw", tables, jnp.concatenate(blocks, 1), preferred_element_type=f32)
        out = jnp.swapaxes(out.astype(bf16).reshape(count, groups, rows, width), 0, 1)
        return [out[i] for i in range(groups)] if split else out
    step = min(width, 256)

    def kernel(*refs):
        table_ref, block_refs = refs[0], refs[1 : 1 + len(blocks)]
        out_refs, joined = refs[1 + len(blocks) : -1], refs[-1]
        for j, ref in enumerate(block_refs):
            joined[j * each : (j + 1) * each, :] = ref[0]
        product = jnp.dot(table_ref[0], joined[...], preferred_element_type=f32)
        for i in range(groups):
            part = product[i * rows : (i + 1) * rows, :].astype(bf16)
            if split:
                out_refs[i][0] = part
            else:
                out_refs[0][i, 0] = part

    if split:
        out_shape = [jax.ShapeDtypeStruct((count, rows, width), bf16)] * groups
        out_specs = [pl.BlockSpec((1, rows, step), lambda t, i: (t, 0, i))] * groups
    else:
        out_shape = jax.ShapeDtypeStruct((groups, count, rows, width), bf16)
        out_specs = pl.BlockSpec((groups, 1, rows, step), lambda t, i: (0, t, 0, i))
    return pl.pallas_call(
        kernel,
        grid=(count, width // step),
        out_shape=out_shape,
        in_specs=[pl.BlockSpec((1, height, depth), lambda t, i: (t, 0, 0))]
        + [pl.BlockSpec((1, each, step), lambda t, i: (t, 0, i))] * len(blocks),
        out_specs=out_specs,
        scratch_shapes=[pltpu.VMEM((depth, step), bf16)],
        cost_estimate=pl.CostEstimate(
            flops=2 * tables.size * width,
            transcendentals=0,
            bytes_accessed=2 * (tables.size + count * (depth + height) * width),
        ),
    )(tables, *blocks)


def expert_in(arrived, down, slopes, turn):
    halves, width, hidden = down.shape
    split = isinstance(arrived, list)
    per = arrived[0].shape[0] if split else arrived.shape[1]
    count = slopes.shape[0] // per * halves
    if not USE_KERNELS:
        whole = (jnp.stack(arrived) if split else arrived).reshape(count // halves, halves, per, width)
        turned = jnp.take(down, (turn[0] + jnp.arange(halves)) % halves, axis=0)
        inner = jnp.einsum("yhrw,hwk->yrk", whole, turned, preferred_element_type=f32)
        return (inner.reshape(-1, hidden) * slopes).astype(bf16)
    step = width // 4
    last = 3

    def kernel(*refs):
        arrived_refs, (down_ref, slope_ref, turn_ref, out_ref, joined, total) = refs[:-6], refs[-6:]
        at = pl.program_id(0)
        part = None
        for h in range(halves):
            for y in range(count // halves):
                i = y * halves + h
                joined[h, y * per : (y + 1) * per, :] = arrived_refs[i][...] if split else arrived_refs[0][i]
            more = jnp.dot(joined[h], down_ref[lax.rem(turn_ref[0] + h, halves)], preferred_element_type=f32)
            part = more if part is None else part + more

        @pl.when(at == 0)
        def _():
            total[...] = part

        @pl.when((at > 0) & (at < last))
        def _():
            total[...] += part

        @pl.when(at == last)
        def _():
            out_ref[...] = ((total[...] + part) * slope_ref[...]).astype(bf16)

    if split:
        specs, operands = [pl.BlockSpec((per, step), lambda i: (0, i))] * count, arrived
    else:
        specs, operands = [pl.BlockSpec((count, per, step), lambda i: (0, 0, i))], [arrived]
    return pl.pallas_call(
        kernel,
        grid=(4,),
        out_shape=jax.ShapeDtypeStruct(slopes.shape, bf16),
        in_specs=specs
        + [
            pl.BlockSpec((halves, step, hidden), lambda i: (0, i, 0)),
            pl.BlockSpec(slopes.shape, lambda i: (0, 0)),
            smem,
        ],
        out_specs=pl.BlockSpec(slopes.shape, lambda i: (0, 0)),
        scratch_shapes=[pltpu.VMEM((halves, count // halves * per, step), bf16), pltpu.VMEM(slopes.shape, f32)],
        cost_estimate=pl.CostEstimate(
            flops=2 * slopes.size * halves * width,
            transcendentals=0,
            bytes_accessed=2 * (count * per * width + down.size) + 6 * slopes.size,
        ),
    )(*operands, down, slopes, turn)


def expert_out(scaled, up, per, split, turn):
    halves, width, hidden = up.shape
    ny = scaled.shape[0] // per
    count = ny * halves
    if not USE_KERNELS:
        turned = jnp.take(up, (turn[0] + jnp.arange(halves)) % halves, axis=0)
        out = jnp.einsum("yrk,hwk->yhrw", scaled.reshape(ny, per, hidden), turned, preferred_element_type=f32)
        out = out.astype(bf16).reshape(count, per, width)
        return [out[i] for i in range(count)] if split else out
    step = width // 4

    def kernel(scaled_ref, up_ref, turn_ref, *out_refs):
        for h in range(halves):
            part = lax.dot_general(
                scaled_ref[...], up_ref[lax.rem(turn_ref[0] + h, halves)], (((1,), (1,)), ((), ())),
                preferred_element_type=f32,
            )
            for y in range(ny):
                rows = part[y * per : (y + 1) * per, :].astype(bf16)
                if split:
                    out_refs[y * halves + h][...] = rows
                else:
                    out_refs[0][y * halves + h] = rows

    if split:
        out_shape = [jax.ShapeDtypeStruct((per, width), bf16)] * count
        out_specs = [pl.BlockSpec((per, step), lambda i: (0, i))] * count
    else:
        out_shape = jax.ShapeDtypeStruct((count, per, width), bf16)
        out_specs = pl.BlockSpec((count, per, step), lambda i: (0, 0, i))
    return pl.pallas_call(
        kernel,
        grid=(4,),
        out_shape=out_shape,
        in_specs=[
            pl.BlockSpec(scaled.shape, lambda i: (0, 0)),
            pl.BlockSpec((halves, step, hidden), lambda i: (0, i, 0)),
            smem,
        ],
        out_specs=out_specs,
        cost_estimate=pl.CostEstimate(
            flops=2 * scaled.size * halves * width,
            transcendentals=0,
            bytes_accessed=2 * (scaled.size + up.size + count * per * width),
        ),
    )(scaled, up, turn)


def gradient(arrived, actives, total, last, turn):
    split = isinstance(arrived, list)
    nt, per, width = arrived[0].shape if split else arrived.shape[1:]
    hidden = actives.shape[2]
    ny = actives.shape[1] // per
    count = len(arrived) if split else arrived.shape[0]
    halves = count // ny
    finish = lambda value: (value * grad_scale).astype(bf16) if last else value
    if not USE_KERNELS:
        whole = (jnp.stack(arrived) if split else arrived).reshape(ny, halves, nt, per, width)
        acts = actives.reshape(nt, ny, per, hidden)
        out = jnp.einsum("yhtrw,tyrk->hwk", whole, acts, preferred_element_type=f32)
        out = jnp.take(out, (turn[0] + jnp.arange(halves)) % halves, axis=0).reshape(halves * width, hidden)
        return finish(out if total is None else out + total)

    def kernel(*refs):
        arrived_refs = refs[: count if split else 1]
        active_ref = refs[len(arrived_refs)]
        turn_ref = refs[len(arrived_refs) + 1]
        total_ref = refs[len(arrived_refs) + 2] if total is not None else None
        out_ref, joined = refs[-2:]
        for h in range(halves):
            for t in range(nt):
                for y in range(ny):
                    at = (t * ny + y) * per
                    i = y * halves + h
                    joined[at : at + per, :] = arrived_refs[i][t] if split else arrived_refs[0][i, t]
            part = lax.dot_general(
                joined[...], active_ref[...].reshape(nt * ny * per, hidden), (((0,), (0,)), ((), ())),
                preferred_element_type=f32,
            )
            rows = pl.ds(pl.multiple_of(lax.rem(turn_ref[0] + h, halves) * width, width), width)
            if total is not None:
                part = part + total_ref[rows, :]
            out_ref[rows, :] = finish(part)

    head = (arrived if split else [arrived]) + [actives]
    operands = head + [turn] + ([] if total is None else [total])
    return pl.pallas_call(
        kernel,
        out_shape=jax.ShapeDtypeStruct((halves * width, hidden), bf16 if last else f32),
        in_specs=[vmem] * len(head) + [smem] + [vmem] * (total is not None),
        out_specs=vmem,
        scratch_shapes=[pltpu.VMEM((nt * ny * per, width), bf16)],
        cost_estimate=pl.CostEstimate(
            flops=2 * count * nt * per * width * hidden,
            transcendentals=0,
            bytes_accessed=2 * (count * nt * per * width + actives.size) + 8 * halves * width * hidden,
        ),
    )(*operands)


def shift(value, axis, by):
    size = lax.axis_size(axis)
    return lax.ppermute(value, axis, [(i, (i + by) % size) for i in range(size)])


def exchange(blocks, sign):
    ny, nc = lax.axis_size("y"), lax.axis_size("c")
    out = [blocks[0]]
    for i in range(1, len(blocks)):
        dy, dc = i // nc, i % nc
        pairs = [
            (y * nc + c, (y + sign * dy) % ny * nc + (c + dc) % nc) for y in range(ny) for c in range(nc)
        ]
        out.append(lax.ppermute(blocks[i], ("y", "c"), pairs))
    return out


def gather_ring(block, odd):
    size = lax.axis_size("z")
    out = [block] + [None] * (size - 1)
    ahead = size // 2 - odd
    held = back = block
    for s in range(1, size // 2 + 1):
        if s <= ahead:
            held = out[size - s] = shift(held, "z", 1)
        if s <= size - 1 - ahead:
            back = out[s] = shift(back, "z", -1)
    return out


def scatter_ring(blocks, odd):
    size = lax.axis_size("z")
    ahead = size // 2 - odd
    add = lambda a, b: (a.astype(f32) + b.astype(f32)).astype(bf16)
    held, back = blocks[ahead], blocks[ahead + 1]
    for s in range(1, size // 2 + 1):
        if s <= ahead:
            held = shift(held, "z", 1)
            if ahead - s > 0:
                held = add(held, blocks[ahead - s])
        if s <= size - 1 - ahead:
            back = shift(back, "z", -1)
            if ahead + 1 + s < size:
                back = add(back, blocks[ahead + 1 + s])
    return (held.astype(f32) + back.astype(f32) + blocks[0].astype(f32)).astype(bf16)


def body(cotangent, expert_ids, gate_values, hidden_pre, up_weight, down_weight):
    ny, nz, nc, nx = (lax.axis_size(a) for a in ("y", "z", "c", "x"))
    own_y, own_z, own_c, own_x = (lax.axis_index(a) for a in ("y", "z", "c", "x"))
    experts = ny * nz * nc
    tokens, top = expert_ids.shape
    width = cotangent.shape[1]
    slots = hidden_pre.shape[1]
    cap = slots // experts
    per = nz * cap
    part = width // nx // nc
    RING = 1

    def halves_of(weight):
        rows = weight.reshape(nx, nc, part, weight.shape[1])
        return jnp.swapaxes(rows, 0, 1).reshape(nc, nx * part, weight.shape[1])

    up, down = halves_of(up_weight[0]), halves_of(down_weight[0])
    turns = [jnp.zeros((1,), jnp.int32), own_c.astype(jnp.int32).reshape(1)]

    def swap(value):
        return lax.all_to_all(value, "c", split_axis=0, concat_axis=0, tiled=True)

    shaped = jnp.moveaxis(cotangent.reshape(tokens, nx, nc, part), 2, 0).reshape(nc, tokens, nx * part)
    start = swap(shaped)

    routes = expert_ids.reshape(-1)
    one_hot = (routes[:, None] == jnp.arange(experts, dtype=jnp.int32)[None, :]).astype(jnp.int32)
    earlier = jnp.cumsum(one_hot, axis=0) - one_hot
    rank = jnp.sum(earlier * one_hot, axis=1)
    code = (routes * cap + rank).reshape(tokens, top)
    meta = jnp.concatenate([code.astype(f32), gate_values], 1).T
    meta = lax.all_to_all(
        jnp.broadcast_to(meta[None], (nz * nc,) + meta.shape), ("z", "c"), split_axis=0, concat_axis=0, tiled=True
    )
    steps = jnp.arange(nz)
    near = jnp.arange(ny * nc)

    def row_codes(s):
        expert_y, expert_c = near // nc, near % nc
        if s == RING:
            expert_y, expert_c = (own_y + expert_y) % ny, (own_c + expert_c) % nc
        expert_of = (expert_y * nz + own_z) * nc + expert_c
        return (
            expert_of[:, None, None] * cap + steps[None, :, None] * slots + jnp.arange(cap)[None, None, :]
        ).reshape(slots, 1)

    def column_side(values, s):
        values = values.reshape(nz, nc, 2 * top, tokens)[:, s]
        codes = values[:, :top].astype(jnp.int32) + steps[:, None, None] * slots
        gates = values[:, top:]
        if s == RING:
            order = (own_z + steps) % nz
            codes, gates = jnp.take(codes, order, axis=0), jnp.take(gates, order, axis=0)
        return codes, gates

    def pick_table(values, s, gated):
        sides = [column_side(v, s) for v in values]
        codes = jnp.stack([jnp.moveaxis(c, 1, 0).reshape(top, 1, nz * tokens) for c, _ in sides])
        gates = jnp.stack([jnp.moveaxis(g, 1, 0).reshape(top, 1, nz * tokens) for _, g in sides])
        row_code = row_codes(s)[None]
        total = jnp.zeros((len(sides), slots, nz * tokens), f32)
        for k in range(top):
            match = row_code == codes[:, k]
            total = total + (jnp.where(match, gates[:, k], 0.0) if gated else match.astype(f32))
        return total.astype(bf16)

    def combine_table(values, s):
        codes, gates = column_side(values, s)
        codes = jnp.moveaxis(codes, 2, 1).reshape(nz * tokens, top)
        gates = jnp.moveaxis(gates, 2, 1).reshape(nz * tokens, top)
        row_code = row_codes(s).reshape(1, slots)
        total = jnp.zeros((nz * tokens, slots), f32)
        for k in range(top):
            total = total + jnp.where(codes[:, k : k + 1] == row_code, gates[:, k : k + 1], 0.0)
        return total.astype(bf16)[None]

    A, B = 0, 1
    picks = [pick_table([meta], s, False) for s in range(nc)]
    combines = [combine_table(meta, s) for s in range(nc)]

    hidden = hidden_pre[0].reshape(ny, nz, nc, cap, hidden_pre.shape[2])
    slopes, actives = [], []
    for s in range(nc):
        rows = hidden[:, :, s]
        if s == RING:
            rows = jnp.take(rows, (own_y - jnp.arange(ny)) % ny, axis=0)
        slope, active = slope_and_act(rows.reshape(ny * per, -1))
        slopes.append(slope)
        actives.append(active)

    def across(rows, sign, s):
        if s == RING:
            return exchange(rows, sign)
        return lax.all_to_all(rows, ("y", "c"), split_axis=0, concat_axis=0, tiled=True)

    def gather(block, s):
        if s == RING:
            return gather_ring(block, 0)
        return [lax.all_gather(block, "z", axis=0, tiled=True)]

    def scatter(parts, s):
        if s == RING:
            return scatter_ring([p[0] for p in parts], 1)
        return lax.psum_scatter(parts.reshape(nz * tokens, -1), "z", scatter_dimension=0, tiled=True)

    def take_rows(s, spread, after):
        spread = [tie(block, after)[None] for block in spread] if after is not None else [b[None] for b in spread]
        rows = table_matmul(picks[s], spread, per, s == RING)
        return [r[0] for r in rows] if s == RING else rows.reshape(ny * nc, per, -1)

    def apply_expert(s, sent, after):
        scaled = expert_in(tie(sent, after), down, slopes[s], turns[s])
        return expert_out(scaled, up, per, s == RING, turns[s])

    def merge(s, back, after):
        back = tie(back, after)
        blocks = [b[None] for b in back] if s == RING else [back.reshape(1, slots, -1)]
        return table_matmul(combines[s], blocks, tokens, s == RING)

    def both_chains(spread, before, early, middle, late):
        rows_a = take_rows(A, spread[A], before)
        sent_a = across(rows_a, 1, A)
        pieces_a = apply_expert(A, sent_a, rows_a)
        back_a = across(pieces_a, -1, A)
        made = early(rows_a, pieces_a)
        rows_b = take_rows(B, spread[B], pieces_a)
        sent_b = across(rows_b, 1, B)
        parts_a = merge(A, back_a, (rows_b, made[0]))
        out_a = scatter(parts_a, A)
        pieces_b = apply_expert(B, sent_b, (parts_a, made[1]))
        back_b = across(pieces_b, -1, B)
        next_a, done = middle(tie(out_a, pieces_b), rows_b)
        parts_b = merge(B, back_b, (pieces_b, done))
        out_b = scatter(parts_b, B)
        return out_a, out_b, next_a, late(out_b), parts_b

    later = {}

    def ask_far(rows, pieces):
        values = tie(meta, pieces)
        far = lax.all_to_all(
            jnp.broadcast_to(values.reshape(1, -1, tokens), (nx, values.size // tokens, tokens)), "x",
            split_axis=0, concat_axis=0, tiled=True,
        )
        later["far"] = far = jnp.take(far, (own_x + jnp.arange(nx)) % nx, axis=0)
        return (), far

    def far_table(s, after):
        values = tie(later["far"], after)
        return pick_table([values[dx] for dx in range(nx)], s, True)

    def early_second(rows, pieces):
        acts = lax.all_gather(tie(jnp.stack(actives), rows), "x", axis=0)
        later["acts"] = jnp.take(acts, (own_x + jnp.arange(nx)) % nx, axis=0)
        later[A] = far_table(A, rows)
        return later["acts"], later[A]

    def send_columns(s, second):
        grad = (start[s].astype(f32) + first[s].astype(f32) + second.astype(f32)).astype(bf16)
        columns = jnp.moveaxis(grad.reshape(tokens, nx, part), 1, 0)
        owned = lax.all_to_all(columns, "x", split_axis=0, concat_axis=0, tiled=True)
        owned = jnp.take(owned, (own_x + jnp.arange(nx)) % nx, axis=0)
        return grad, owned, gather(owned.reshape(nx * tokens, part), s)

    def middle_second(second, rows_b):
        grad, owned, spread = send_columns(A, second)
        later[B] = far_table(B, rows_b)
        return (grad, spread), (owned, later[B])

    spread = [gather(start[A], A), None]
    whole = lax.all_gather(tie(start[B], meta), "z", axis=0, tiled=True).reshape(nz, tokens, -1)
    spread[B] = [jnp.take(whole, (own_z + steps) % nz, axis=0).reshape(nz * tokens, -1)]
    first_a, first_b, spread_a, spread_b, last = both_chains(
        spread, None, ask_far,
        lambda out, rows: (gather(out, A), None), lambda out: gather(out, B),
    )
    first = [first_a, first_b]
    _, _, (grad_a, spread_a), (grad_b, _, spread_b), last = both_chains(
        [spread_a, spread_b], last, early_second, middle_second, lambda out: send_columns(B, out)
    )
    own_grads, spread = [grad_a, grad_b], [spread_a, spread_b]
    own = swap(jnp.stack(own_grads))
    input_grad = jnp.moveaxis(own.reshape(nc, tokens, nx, part), 0, 2).reshape(tokens, width)
    arrived = []
    for s in range(nc):
        if s == RING:
            blocks = [b.reshape(nx, tokens, part) for b in spread[s]]
        else:
            blocks = list(spread[s][0].reshape(nz, nx, tokens, part))
        rows = table_matmul(later[s], blocks, per, s == RING)
        if s != RING:
            rows = rows.reshape(ny * nc, nx * per, part)
        got = across(rows, 1, s)
        arrived.append(got if s == RING else got.reshape(ny * nc, nx, per, part))
    total = gradient(arrived[A], later["acts"][:, A], None, False, turns[A])
    total = gradient(arrived[B], later["acts"][:, B], total, True, turns[B])
    return input_grad, total[None]


def solution(mesh):
    axes = ("y", "z", "c", "x")
    count_z, count_c = 8, 2
    grid = mesh.devices.reshape(-1, count_z, count_c, mesh.devices.shape[1])
    inner_mesh = Mesh(grid, axes)
    in_specs = (
        P(axes, None),
        P(axes, None),
        P(axes, None),
        P(axes[:3], "x", None),
        P(axes[:3], None, None),
        P(axes[:3], None, None),
    )
    out_specs = (P(axes, None), P(axes[:3], "x", None))

    return jax.shard_map(body, mesh=inner_mesh, in_specs=in_specs, out_specs=out_specs, check_vma=False)
```
